32 devices in a mesh: pgroup: 8 (over y, x, core), tile: 4 (over z).
Axes of the slice: x: 2, y: 2, z: 4, core: 2. Of those that a mesh axis runs over, the one named last changes fastest.
Arguments:
- images: float32 [64, 256, 2048], P(('pgroup', 'tile')), may hold values from -6 to 6
- beams: float32 [64, 256, 2048], P(('pgroup', 'tile')), may hold values from 0.2 to 1
- row_block: int32 [64], P(('pgroup', 'tile')), may hold values from 0 to 14, as said below
- col_block: int32 [64], P(('pgroup', 'tile')), may hold values from 0 to 16
- band: int32 [64, 2], P(('pgroup', 'tile')), may hold values from 0 to 3
- row_frac: float32 [64], P(('pgroup', 'tile')), may hold values from 0.05 to 0.95
- col_frac: float32 [64], P(('pgroup', 'tile')), may hold values from 0.05 to 0.95
Outputs:
- numer: float32 [2048, 4096], P('tile', 'pgroup')
- weight: float32 [2048, 4096], P('tile', 'pgroup')
- normalised: float32 [2048, 4096], P('tile', 'pgroup')
The draws below stay inside these ranges and needn't reach their ends.
Inputs may be any that keep to these rules, and one draw needn't show every extreme that they name: With t = (p // 2) mod 4, row_block[p] - 4 t lies in 0 to 2, and the largest value is taken in every draw.
All inputs are finite; a program needn't handle non-finite values.
Results may differ from the reference program's by a relative error of at most 0.00002.
Values sent between devices are 32-bit elements; how exact they have to be, the bound alone decides.
A program may use at most 128 MiB of HBM per device.

```python
import math
import jax
import jax.numpy as jnp
from jax import lax

W = 2048
IMG_ROWS = 256
IMG_BLOCKS = 2
PTS_DEV = 2
POINTINGS = 64
TILE_BLOCKS = 4
SKY_ROWS = 2048
SKY_COLS = 4096
HALO = 4
N_TILE = 4


def draw_row_block(key, part):
    pointing = jnp.arange(POINTINGS, dtype=jnp.int32)
    owner = pointing // PTS_DEV % N_TILE
    offset = jax.random.randint(key, (POINTINGS,), 0, TILE_BLOCKS - IMG_BLOCKS + 1, dtype=jnp.int32)
    offset = offset.at[0].set(TILE_BLOCKS - IMG_BLOCKS)
    return owner * TILE_BLOCKS + offset


def place_ends(array, own_key, low, high):
    index_at = [jax.random.randint(jax.random.fold_in(own_key, axis), (), 0, length) for axis, length in enumerate(array.shape)]
    widest = array.shape.index(max(array.shape))
    next_to = index_at[:widest] + [(index_at[widest] + 1) % array.shape[widest]] + index_at[widest + 1:]
    return array.at[tuple(index_at)].set(low).at[tuple(next_to)].set(high)


def level_of(own_key, shape, shards, least, largest):
    factor_of = 1.0
    for dim, blocks in shards:
        draws = jax.random.uniform(jax.random.fold_in(jax.random.fold_in(own_key, 6), dim), (blocks,), jnp.float32, least / len(shards), largest / len(shards))
        factor_of = factor_of * jnp.repeat(jnp.exp(draws), shape[dim] // blocks).reshape((-1,) + (1,) * (len(shape) - 1 - dim))
    return factor_of


def centred(rng, dims, width, reach, cuts=(), kind=jnp.bfloat16):
    level = level_of(rng, dims, cuts, -0.22, 0.18) if cuts else 1.0
    entries = jax.random.normal(rng, dims, jnp.float32) * width * level
    return jnp.minimum(jnp.maximum(entries, -reach), reach).astype(kind)


def setup_inputs(seed: int = 0) -> dict:
    key_list = jax.random.split(jax.random.key(seed), 8)
    return {
        "images": centred(key_list[0], (POINTINGS, IMG_ROWS, W), 1.0, 6.0, ((0, 32),), jnp.float32),
        "beams": jnp.clip(jnp.exp(math.log(1.0) - 1.609438 * jax.random.uniform(key_list[1], (POINTINGS, IMG_ROWS, W), jnp.float32) ** level_of(key_list[1], (POINTINGS, IMG_ROWS, W), ((0, 32),), -0.2, 0.2)), 0.2, 1.0),
        "row_block": draw_row_block(jax.random.fold_in(key_list[7], 71), 0),
        "col_block": place_ends(jax.random.randint(key_list[3], (POINTINGS,), 0, (SKY_COLS - W) // 128 + 1), jax.random.fold_in(key_list[3], 1), 0, ((SKY_COLS - W) // 128 + 1) - 1).astype(jnp.int32),
        "band": place_ends(jax.random.randint(key_list[4], (POINTINGS, IMG_BLOCKS), 0, HALO), jax.random.fold_in(key_list[4], 1), 0, HALO - 1).astype(jnp.int32),
        "row_frac": jnp.clip(0.05 + 0.9 * jax.random.uniform(key_list[5], (POINTINGS,), jnp.float32) ** level_of(key_list[5], (POINTINGS,), ((0, 32),), -0.2, 0.2), 0.05, 0.95),
        "col_frac": jnp.clip(0.05 + 0.9 * jax.random.uniform(key_list[6], (POINTINGS,), jnp.float32) ** level_of(key_list[6], (POINTINGS,), ((0, 32),), -0.2, 0.2), 0.05, 0.95),
    }


def contribution(image_block, beam_block, shift, row_f, col_f):
    stacked = jnp.stack([beam_block * image_block, beam_block * beam_block])
    moved = jnp.concatenate([jnp.zeros_like(stacked[:, :, :1]), stacked[:, :, :-1]], axis=2)
    banded = (1.0 - col_f) * stacked + col_f * moved
    empty = jnp.zeros((2, 128 + HALO, banded.shape[2]), jnp.float32)
    zero = jnp.int32(0)
    first = lax.dynamic_update_slice(empty, (1.0 - row_f) * banded, (zero, shift.astype(jnp.int32), zero))
    second = lax.dynamic_update_slice(empty, row_f * banded, (zero, (shift + 1).astype(jnp.int32), zero))
    return first + second


def reference(images, beams, row_block, col_block, band, row_frac, col_frac):
    canvas = jnp.zeros((2, SKY_ROWS + 128 + HALO, SKY_COLS), jnp.float32)

    def visit(index, canvas):
        for block in range(IMG_BLOCKS):
            image_block = lax.dynamic_slice_in_dim(images[index], block * 128, 128, 0)
            beam_block = lax.dynamic_slice_in_dim(beams[index], block * 128, 128, 0)
            piece = contribution(image_block, beam_block, band[index, block], row_frac[index], col_frac[index])
            row_start = ((row_block[index] + block) * 128).astype(jnp.int32)
            col_start = (col_block[index] * 128).astype(jnp.int32)
            zero = jnp.int32(0)
            old = lax.dynamic_slice(canvas, (zero, row_start, col_start), piece.shape)
            canvas = lax.dynamic_update_slice(canvas, old + piece, (zero, row_start, col_start))
        return canvas

    canvas = lax.fori_loop(0, POINTINGS, visit, canvas)
    numer = canvas[0, :SKY_ROWS]
    weight = canvas[1, :SKY_ROWS]
    normalised = numer / jnp.maximum(weight, 0.05)
    return numer, weight, normalised
```

```python
import functools
import math

import jax
import jax.numpy as jnp
from jax import lax
from jax.experimental import pallas as pl
from jax.experimental.pallas import tpu as pltpu
from jax.sharding import PartitionSpec as P

TILE_BLOCKS = 4
SKY_COLS = 4096
HALO = 4
LANES = 128
BLOCK = 128
ROWS = 64
TALL = BLOCK + 8
MESH = pl.DeviceIdType.MESH
F32 = jnp.float32


def chip_grid(groups):
    chips = groups // 2
    along_x = math.isqrt(chips)
    while chips % along_x:
        along_x -= 1
    return chips // along_x, along_x


def kernel(
    ny, nx, n_tile,
    images, beams, row_block, col_block, band, row_frac, col_frac,
    out,
    raw_i, raw_b, mid, placed, halo_out, halo_in, give, take, canvas,
    first_a, first_b, second_a, second_b, last,
    load_sem, halo_sem, swap_sem, first_sem, second_sem, last_sem,
):
    points, img_rows, width = images.shape
    blocks = img_rows // BLOCK
    col_tiles = width // LANES
    sky_tiles = SKY_COLS // LANES
    own = sky_tiles // (ny * nx)
    half = own // 2
    pairs = TILE_BLOCKS
    per_array = points * blocks * col_tiles
    empty = 2 * per_array

    me = lax.axis_index("pgroup")
    tile = lax.axis_index("tile")
    core = lax.rem(me, 2)
    chip = me // 2
    x = lax.rem(chip, nx)
    y = chip // nx
    partner = me + 1 - 2 * core
    x_peers = [(y * nx + lax.rem(x + d, nx)) * 2 + core for d in range(1, nx)]
    y_peers = [(lax.rem(y + d, ny) * nx + x) * 2 + core for d in range(1, ny)]
    after = lax.rem(tile + 1, n_tile)
    before = lax.rem(tile + n_tile - 1, n_tile)

    loads = []
    for p in range(points):
        for b in range(blocks):
            for which, (source, target) in enumerate(((images, raw_i), (beams, raw_b))):
                rows = pl.ds(b * BLOCK, BLOCK)
                copy = pltpu.make_async_copy(
                    source.at[p, rows], target.at[p, rows], load_sem.at[which, p * blocks + b]
                )
                copy.start()
                loads.append(copy)

    barrier = pltpu.get_barrier_semaphore()
    near = [{"pgroup": q} for q in [partner] + x_peers + y_peers]
    near += [{"tile": after}, {"tile": before}]
    for device in near:
        pl.semaphore_signal(barrier, inc=1, device_id=device, device_id_type=MESH)

    placed[empty] = jnp.zeros((TALL, LANES), F32)
    for slot in range(4):
        mid[slot, :8] = jnp.zeros((8, LANES), F32)
        mid[slot, 8 + BLOCK :] = jnp.zeros((8, LANES), F32)
    first_lane = lax.broadcasted_iota(jnp.int32, (BLOCK, LANES), 1) == 0

    for p in range(points):
        f = row_frac[p]
        g = col_frac[p]
        for b in range(blocks):
            loads[2 * (p * blocks + b)].wait()
            loads[2 * (p * blocks + b) + 1].wait()
            shift = band[p, b]
            rows = pl.ds(b * BLOCK, BLOCK)

            def tile_pair(step, _, p=p, b=b, f=f, g=g, shift=shift, rows=rows):
                for sub in range(2):
                    t = 2 * step + sub
                    lanes = pl.ds(pl.multiple_of(t * LANES, LANES), LANES)
                    left = pl.ds(pl.multiple_of(jnp.maximum(t - 1, 0) * LANES, LANES), LANES)
                    there = jnp.where(t > 0, g, 0.0)
                    beam = raw_b[p, rows, lanes]
                    beam_left = raw_b[p, rows, left]
                    for a, other in enumerate((raw_i, raw_b)):
                        here = beam * other[p, rows, lanes]
                        prior = beam_left * other[p, rows, left]
                        moved = jnp.where(
                            first_lane,
                            there * pltpu.roll(prior, 1, 1),
                            g * pltpu.roll(here, 1, 1),
                        )
                        slot = 2 * sub + a
                        mid[slot, 8 : 8 + BLOCK] = (1.0 - g) * here + moved
                        low = mid[slot, pl.ds(8 - shift, TALL)]
                        high = mid[slot, pl.ds(7 - shift, TALL)]
                        index = a * per_array + (p * blocks + b) * col_tiles + t
                        placed[index] = (1.0 - f) * low + f * high
                return 0

            lax.fori_loop(0, col_tiles // 2, tile_pair, 0)

    def where_placed(a, p, sky_block, sky_tile):
        b = sky_block - (row_block[p] - tile * TILE_BLOCKS)
        t = sky_tile - col_block[p]
        inside = (b >= 0) & (b < blocks) & (t >= 0) & (t < col_tiles)
        index = a * per_array + (p * blocks + b) * col_tiles + t
        return jnp.where(inside, index, empty)

    def slot_of(sky_tile, x_major):
        if not x_major:
            return sky_tile
        owner = sky_tile // own
        return (lax.rem(owner, nx) * ny + owner // nx) * own + lax.rem(sky_tile, own)

    def gather(a, sky_block, sky_tile, lower):
        start = ROWS if lower else 0
        total = None
        for p in range(points):
            term = placed[where_placed(a, p, sky_block, sky_tile), start : start + ROWS]
            total = term if total is None else total + term
        if lower:
            return total, None
        top = total[:8]
        for p in range(points):
            top = top + placed[where_placed(a, p, sky_block - 1, sky_tile), BLOCK:TALL]
        return total, top

    def border(sky_tile, _):
        for a in range(2):
            top = None
            for p in range(points):
                term = placed[where_placed(a, p, TILE_BLOCKS - 1, sky_tile), BLOCK:TALL]
                top = term if top is None else top + term
            halo_out[a, sky_tile] = top
        return 0

    lax.fori_loop(0, sky_tiles, border, 0)
    pl.semaphore_wait(barrier, len(near))

    halo = pltpu.make_async_remote_copy(
        halo_out, halo_in, halo_sem.at[0], halo_sem.at[1],
        device_id={"tile": after}, device_id_type=MESH,
    )
    halo.start()

    def swap(k):
        return pltpu.make_async_remote_copy(
            give.at[k], take.at[k], swap_sem.at[0, k], swap_sem.at[1, k],
            device_id={"pgroup": partner}, device_id_type=MESH,
        )

    def build(k, j, lower):
        sky_block = pairs - 1 - j
        other = 1 - core

        def one(sky_tile, _):
            total, top = gather(other, sky_block, sky_tile, lower)
            slot = slot_of(sky_tile, lower)
            give[k, slot] = total
            if top is not None:
                give[k, slot, :8] = top
            return 0

        lax.fori_loop(0, sky_tiles, one, 0, unroll=2)
        if not lower:
            @pl.when(j == pairs - 1)
            def _():
                halo.wait_recv()
                use = jnp.where(tile > 0, 1.0, 0.0)

                def add(s, _):
                    give[k, s, :8] += use * halo_in[other, s]
                    return 0

                lax.fori_loop(0, sky_tiles, add, 0, unroll=4)
        swap(k).start()

    def first_copies(k, j, lower):
        copies = []
        count, at, peers = (nx, x, x_peers) if lower else (ny, y, y_peers)
        size = sky_tiles // count
        target = first_a if lower else first_b
        for d in range(1, count):
            to = lax.rem(at + d, count)
            copies.append(pltpu.make_async_remote_copy(
                canvas.at[k, pl.ds(to * size, size)], target.at[j, d - 1],
                first_sem.at[0, k, d - 1], first_sem.at[1, k, d - 1],
                device_id={"pgroup": peers[d - 1]}, device_id_type=MESH,
            ))
        return copies

    def second_copies(k, j, lower):
        copies = []
        count, at, peers = (ny, y, y_peers) if lower else (nx, x, x_peers)
        base = (x * ny if lower else y * nx) * own
        target = second_a if lower else second_b
        for d in range(1, count):
            to = lax.rem(at + d, count)
            copies.append(pltpu.make_async_remote_copy(
                canvas.at[k, pl.ds(base + to * own, own)], target.at[j, d - 1],
                second_sem.at[0, k, d - 1], second_sem.at[1, k, d - 1],
                device_id={"pgroup": peers[d - 1]}, device_id_type=MESH,
            ))
        return copies

    def combine(k, j, lower):
        sky_block = pairs - 1 - j
        swap(k).wait_recv()

        def one(sky_tile, _):
            total, top = gather(core, sky_block, sky_tile, lower)
            slot = slot_of(sky_tile, lower)
            canvas[k, slot] = total + take[k, slot]
            if top is not None:
                canvas[k, slot, :8] = top + take[k, slot, :8]
            return 0

        lax.fori_loop(0, sky_tiles, one, 0, unroll=2)
        if not lower:
            @pl.when(j == pairs - 1)
            def _():
                use = jnp.where(tile > 0, 1.0, 0.0)

                def add(s, _):
                    canvas[k, s, :8] += use * halo_in[core, s]
                    return 0

                lax.fori_loop(0, sky_tiles, add, 0, unroll=4)
        for copy in first_copies(k, j, lower):
            copy.start()

    build(0, 0, True)
    build(1, 0, False)

    def spread(j, _):
        for lower in (True, False):
            k = 2 * j + (0 if lower else 1)
            combine(k, j, lower)

            @pl.when(j < pairs - 1)
            def _():
                build(k + 2, j + 1, lower)
        return 0

    lax.fori_loop(0, pairs, spread, 0)

    def middle(j, _):
        for lower in (True, False):
            k = 2 * j + (0 if lower else 1)
            copies = first_copies(k, j, lower)
            for copy in copies:
                copy.wait_recv()
            count, at = (nx, x) if lower else (ny, y)
            size = sky_tiles // count
            source = first_a if lower else first_b

            def one(s, _):
                total = canvas[k, at * size + s]
                for d in range(count - 1):
                    total = total + source[j, d, s]
                canvas[k, at * size + s] = total
                return 0

            lax.fori_loop(0, size, one, 0, unroll=2)
            for copy in second_copies(k, j, lower):
                copy.start()
        return 0

    lax.fori_loop(0, pairs, middle, 0)

    def mine(lower):
        return (x * ny + y if lower else y * nx + x) * own

    def last_copy(k, lower):
        return pltpu.make_async_remote_copy(
            canvas.at[k, pl.ds(mine(lower) + (1 - core) * half, half)], last.at[k],
            last_sem.at[0, k], last_sem.at[1, k],
            device_id={"pgroup": partner}, device_id_type=MESH,
        )

    def finish(j, _):
        for lower in (True, False):
            k = 2 * j + (0 if lower else 1)
            for copy in second_copies(k, j, lower):
                copy.wait_recv()
            source = second_a if lower else second_b
            count = ny if lower else nx
            row = (pairs - 1 - j) * BLOCK + (ROWS if lower else 0)
            rows = pl.ds(pl.multiple_of(row, ROWS), ROWS)

            def summed(s):
                total = canvas[k, mine(lower) + s]
                for d in range(count - 1):
                    total = total + source[j, d, s]
                return total

            for s in range(half):
                canvas[k, mine(lower) + (1 - core) * half + s] = summed((1 - core) * half + s)
            last_copy(k, lower).start()
            for s in range(half):
                out[core, rows, s * LANES : (s + 1) * LANES] = summed(core * half + s)
        return 0

    lax.fori_loop(0, pairs, finish, 0)

    def receive(j, _):
        for lower in (True, False):
            k = 2 * j + (0 if lower else 1)
            last_copy(k, lower).wait()
            row = (pairs - 1 - j) * BLOCK + (ROWS if lower else 0)
            rows = pl.ds(pl.multiple_of(row, ROWS), ROWS)
            for s in range(half):
                out[1 - core, rows, s * LANES : (s + 1) * LANES] = last[k, s]
            swap(k).wait_send()
            for copy in first_copies(k, j, lower) + second_copies(k, j, lower):
                copy.wait_send()
        return 0

    lax.fori_loop(0, pairs, receive, 0)
    halo.wait_send()


def body(ny, nx, n_tile, images, beams, row_block, col_block, band, row_frac, col_frac):
    points, img_rows, width = images.shape
    blocks = img_rows // BLOCK
    col_tiles = width // LANES
    sky_tiles = SKY_COLS // LANES
    own = sky_tiles // (ny * nx)
    pairs = TILE_BLOCKS
    chunks = 2 * pairs
    own_cols = SKY_COLS // (2 * ny * nx)
    most = max(nx, ny) - 1
    dma = pltpu.SemaphoreType.DMA
    smem = pl.BlockSpec(memory_space=pltpu.SMEM)
    summed = pl.pallas_call(
        functools.partial(kernel, ny, nx, n_tile),
        out_shape=jax.ShapeDtypeStruct((2, TILE_BLOCKS * BLOCK, own_cols), F32),
        in_specs=[pl.BlockSpec(memory_space=pl.ANY)] * 2 + [smem] * 5,
        out_specs=pl.BlockSpec(memory_space=pltpu.VMEM),
        scratch_shapes=[
            pltpu.VMEM((points, img_rows, width), F32),
            pltpu.VMEM((points, img_rows, width), F32),
            pltpu.VMEM((4, BLOCK + 16, LANES), F32),
            pltpu.VMEM((2 * points * blocks * col_tiles + 1, TALL, LANES), F32),
            pltpu.VMEM((2, sky_tiles, 8, LANES), F32),
            pltpu.VMEM((2, sky_tiles, 8, LANES), F32),
            pltpu.VMEM((chunks, sky_tiles, ROWS, LANES), F32),
            pltpu.VMEM((chunks, sky_tiles, ROWS, LANES), F32),
            pltpu.VMEM((chunks, sky_tiles, ROWS, LANES), F32),
            pltpu.VMEM((pairs, nx - 1, sky_tiles // nx, ROWS, LANES), F32),
            pltpu.VMEM((pairs, ny - 1, sky_tiles // ny, ROWS, LANES), F32),
            pltpu.VMEM((pairs, ny - 1, own, ROWS, LANES), F32),
            pltpu.VMEM((pairs, nx - 1, own, ROWS, LANES), F32),
            pltpu.VMEM((chunks, own // 2, ROWS, LANES), F32),
            dma((2, points * blocks)),
            dma((2,)),
            dma((2, chunks)),
            dma((2, chunks, most)),
            dma((2, chunks, most)),
            dma((2, chunks)),
        ],
        compiler_params=pltpu.CompilerParams(
            collective_id=0, has_side_effects=True, vmem_limit_bytes=67043328
        ),
        name="combine",
    )(images, beams, row_block, col_block, band, row_frac, col_frac)
    numer = summed[0]
    weight = summed[1]
    normalised = numer / jnp.maximum(weight, 0.05)
    return (numer, weight, normalised)


def solution(mesh):
    ny, nx = chip_grid(mesh.shape["pgroup"])
    return jax.shard_map(
        functools.partial(body, ny, nx, mesh.shape["tile"]),
        mesh=mesh,
        in_specs=(
            P(("pgroup", "tile"), None, None),
            P(("pgroup", "tile"), None, None),
            P(("pgroup", "tile")),
            P(("pgroup", "tile")),
            P(("pgroup", "tile"), None),
            P(("pgroup", "tile")),
            P(("pgroup", "tile")),
        ),
        out_specs=(P("tile", "pgroup"), P("tile", "pgroup"), P("tile", "pgroup")),
        check_vma=False,
    )
```

```python
import functools
import math

import jax
import jax.numpy as jnp
from jax import lax
from jax.experimental import pallas as pl
from jax.experimental.pallas import tpu as pltpu
from jax.sharding import PartitionSpec as P

TILE_BLOCKS = 4
SKY_COLS = 4096
HALO = 4
LANES = 128
BLOCK = 128
ROWS = 32
PER_BLOCK = BLOCK // (2 * ROWS)
TALL = BLOCK + 8
AHEAD = 2
LAG = 2
MESH = pl.DeviceIdType.MESH
F32 = jnp.float32


def chip_grid(groups):
    chips = groups // 2
    along_x = math.isqrt(chips)
    while chips % along_x:
        along_x -= 1
    return chips // along_x, along_x


def kernel(
    ny, nx, n_tile,
    images, beams, row_block, col_block, band, row_frac, col_frac,
    out,
    raw, mid, placed, halo_out, halo_in, give, take, canvas,
    first_a, first_b, second_a, second_b, last,
    ready,
    load_sem, halo_sem, swap_sem, first_sem, second_sem, last_sem, out_sem,
):
    points, img_rows, width = images.shape
    blocks = img_rows // BLOCK
    col_tiles = width // LANES
    sky_tiles = SKY_COLS // LANES
    own = sky_tiles // (ny * nx)
    half = own // 2
    pairs = TILE_BLOCKS * PER_BLOCK
    per_array = points * blocks * col_tiles
    empty = 2 * per_array

    me = lax.axis_index("pgroup")
    tile = lax.axis_index("tile")
    core = lax.rem(me, 2)
    chip = me // 2
    x = lax.rem(chip, nx)
    y = chip // nx
    partner = me + 1 - 2 * core
    x_peers = [(y * nx + lax.rem(x + d, nx)) * 2 + core for d in range(1, nx)]
    y_peers = [(lax.rem(y + d, ny) * nx + x) * 2 + core for d in range(1, ny)]
    after = lax.rem(tile + 1, n_tile)
    before = lax.rem(tile + n_tile - 1, n_tile)

    loads = {}
    for b in reversed(range(blocks)):
        for p in range(points):
            for which, source in enumerate((images, beams)):
                rows = pl.ds(b * BLOCK, BLOCK)
                copy = pltpu.make_async_copy(
                    source.at[p, rows], raw.at[which, p, rows], load_sem.at[which, p * blocks + b]
                )
                copy.start()
                loads[which, p, b] = copy

    barrier = pltpu.get_barrier_semaphore()
    near = [{"pgroup": q} for q in [partner] + x_peers + y_peers]
    near += [{"tile": after}, {"tile": before}]
    for device in near:
        pl.semaphore_signal(barrier, inc=1, device_id=device, device_id_type=MESH)

    placed[empty] = jnp.zeros((TALL, LANES), F32)
    for slot in range(4):
        mid[slot, :8] = jnp.zeros((8, LANES), F32)
        mid[slot, 8 + BLOCK :] = jnp.zeros((8, LANES), F32)
    last_lane = lax.broadcasted_iota(jnp.int32, (BLOCK, LANES), 1) == LANES - 1

    def interpolate(a, fresh, some):
        for b in some:
            for p in range(points):
                f = row_frac[p]
                g = col_frac[p]
                if fresh:
                    loads[0, p, b].wait()
                    loads[1, p, b].wait()
                shift = band[p, b]
                rows = pl.ds(b * BLOCK, BLOCK)

                def some_tiles(step, _, p=p, b=b, f=f, g=g, shift=shift, rows=rows):
                    for sub in range(4):
                        t = 4 * step + sub
                        lanes = pl.ds(pl.multiple_of(t * LANES, LANES), LANES)
                        here = raw[1, p, rows, lanes] * raw[a, p, rows, lanes]
                        if sub == 0:
                            left = pl.ds(pl.multiple_of(jnp.maximum(t - 1, 0) * LANES, LANES), LANES)
                            there = jnp.where(t > 0, 1.0, 0.0)
                            prior = raw[1, p, rows, left] * raw[a, p, rows, left] * there
                        else:
                            left = pl.ds(pl.multiple_of((t - 1) * LANES, LANES), LANES)
                            prior = raw[1, p, rows, left] * raw[a, p, rows, left]
                        moved = pltpu.roll(jnp.where(last_lane, prior, here), 1, 1)
                        mid[sub, 8 : 8 + BLOCK] = (1.0 - g) * here + g * moved
                        low = mid[sub, pl.ds(8 - shift, TALL)]
                        high = mid[sub, pl.ds(7 - shift, TALL)]
                        index = a * per_array + (p * blocks + b) * col_tiles + t
                        placed[index] = (1.0 - f) * low + f * high
                    return 0

                lax.fori_loop(0, col_tiles // 4, some_tiles, 0)

    def where_placed(a, p, sky_block, sky_tile):
        b = sky_block - (row_block[p] - tile * TILE_BLOCKS)
        t = sky_tile - col_block[p]
        inside = (b >= 0) & (b < blocks) & (t >= 0) & (t < col_tiles)
        index = a * per_array + (p * blocks + b) * col_tiles + t
        return jnp.where(inside, index, empty)

    def slot_of(sky_tile, x_major):
        if not x_major:
            return sky_tile
        owner = sky_tile // own
        return (lax.rem(owner, nx) * ny + owner // nx) * own + lax.rem(sky_tile, own)

    def place_of(m, lower):
        m = jnp.int32(m)
        sky_block = TILE_BLOCKS - 1 - m // PER_BLOCK
        turn = lax.rem(m, PER_BLOCK)
        start = BLOCK - ROWS * (2 * turn + (1 if lower else 2))
        return sky_block, pl.multiple_of(start, ROWS)

    def gather(a, m, sky_tile, lower):
        sky_block, start = place_of(m, lower)
        total = None
        for p in range(points):
            term = placed[where_placed(a, p, sky_block, sky_tile), pl.ds(start, ROWS)]
            total = term if total is None else total + term
        if lower:
            return total, None
        top = total[:8]
        for p in range(points):
            index = jnp.where(start == 0, where_placed(a, p, sky_block - 1, sky_tile), empty)
            top = top + placed[index, BLOCK:TALL]
        return total, top

    def border(sky_tile, _):
        for a in range(2):
            top = None
            for p in range(points):
                term = placed[where_placed(a, p, TILE_BLOCKS - 1, sky_tile), BLOCK:TALL]
                top = term if top is None else top + term
            halo_out[a, sky_tile] = top
        return 0

    halo = pltpu.make_async_remote_copy(
        halo_out, halo_in, halo_sem.at[0], halo_sem.at[1],
        device_id={"tile": after}, device_id_type=MESH,
    )

    def swap(k):
        return pltpu.make_async_remote_copy(
            give.at[k], take.at[k], swap_sem.at[0, k], swap_sem.at[1, k],
            device_id={"pgroup": partner}, device_id_type=MESH,
        )

    def build(k, j, lower):
        other = 1 - core

        def one(sky_tile, _):
            total, top = gather(other, j, sky_tile, lower)
            slot = slot_of(sky_tile, lower)
            give[k, slot] = total
            if top is not None:
                give[k, slot, :8] = top
            return 0

        lax.fori_loop(0, sky_tiles, one, 0, unroll=2)
        if not lower:
            @pl.when(jnp.int32(j) == pairs - 1)
            def _():
                halo.wait_recv()
                use = jnp.where(tile > 0, 1.0, 0.0)

                def add(s, _):
                    give[k, s, :8] += use * halo_in[other, s]
                    return 0

                lax.fori_loop(0, sky_tiles, add, 0, unroll=4)
        swap(k).start()

    def first_copies(k, j, lower):
        copies = []
        count, at, peers = (nx, x, x_peers) if lower else (ny, y, y_peers)
        size = sky_tiles // count
        target = first_a if lower else first_b
        for d in range(1, count):
            to = lax.rem(at + d, count)
            copies.append(pltpu.make_async_remote_copy(
                canvas.at[k, pl.ds(to * size, size)], target.at[j, d - 1],
                first_sem.at[0, k, d - 1], first_sem.at[1, k, d - 1],
                device_id={"pgroup": peers[d - 1]}, device_id_type=MESH,
            ))
        return copies

    def second_copies(k, j, lower):
        copies = []
        count, at, peers = (ny, y, y_peers) if lower else (nx, x, x_peers)
        base = (x * ny if lower else y * nx) * own
        target = second_a if lower else second_b
        for d in range(1, count):
            to = lax.rem(at + d, count)
            copies.append(pltpu.make_async_remote_copy(
                canvas.at[k, pl.ds(base + to * own, own)], target.at[j, d - 1],
                second_sem.at[0, k, d - 1], second_sem.at[1, k, d - 1],
                device_id={"pgroup": peers[d - 1]}, device_id_type=MESH,
            ))
        return copies

    def combine(k, j, lower):
        swap(k).wait_recv()

        def one(sky_tile, _):
            total, top = gather(core, j, sky_tile, lower)
            slot = slot_of(sky_tile, lower)
            canvas[k, slot] = total + take[k, slot]
            if top is not None:
                canvas[k, slot, :8] = top + take[k, slot, :8]
            return 0

        lax.fori_loop(0, sky_tiles, one, 0, unroll=2)
        if not lower:
            @pl.when(jnp.int32(j) == pairs - 1)
            def _():
                use = jnp.where(tile > 0, 1.0, 0.0)

                def add(s, _):
                    canvas[k, s, :8] += use * halo_in[core, s]
                    return 0

                lax.fori_loop(0, sky_tiles, add, 0, unroll=4)
        for copy in first_copies(k, j, lower):
            copy.start()

    groups = [[blocks - 1], list(reversed(range(blocks - 1)))]
    interpolate(1 - core, True, groups[0])
    pl.semaphore_wait(barrier, len(near))
    build(0, 0, True)
    build(1, 0, False)
    interpolate(core, False, groups[0])
    combine(0, 0, True)
    combine(1, 0, False)
    interpolate(1 - core, True, groups[1])
    for m in range(1, 1 + AHEAD):
        build(2 * m, m, True)
        build(2 * m + 1, m, False)
    interpolate(core, False, groups[1])

    def spread(j, _):
        for lower in (True, False):
            combine(2 * j + (0 if lower else 1), j, lower)

        @pl.when(j == 1)
        def _():
            lax.fori_loop(0, sky_tiles, border, 0)
            halo.start()

        @pl.when(j < pairs - AHEAD)
        def _():
            for lower in (True, False):
                build(2 * (j + AHEAD) + (0 if lower else 1), j + AHEAD, lower)
        return 0

    lax.fori_loop(1, pairs, spread, 0)

    def middle(j, _):
        for lower in (True, False):
            k = 2 * j + (0 if lower else 1)
            copies = first_copies(k, j, lower)
            for copy in copies:
                copy.wait_recv()
            count, at = (nx, x) if lower else (ny, y)
            size = sky_tiles // count
            source = first_a if lower else first_b

            def one(s, _):
                total = canvas[k, at * size + s]
                for d in range(count - 1):
                    total = total + source[j, d, s]
                canvas[k, at * size + s] = total
                return 0

            lax.fori_loop(0, size, one, 0, unroll=2)
            for copy in second_copies(k, j, lower):
                copy.start()
            swap(k).wait_send()
        return 0

    lax.fori_loop(0, pairs, middle, 0)

    def mine(lower):
        return (x * ny + y if lower else y * nx + x) * own

    def last_copy(k, lower):
        return pltpu.make_async_remote_copy(
            canvas.at[k, pl.ds(mine(lower) + (1 - core) * half, half)], last.at[k],
            last_sem.at[0, k], last_sem.at[1, k],
            device_id={"pgroup": partner}, device_id_type=MESH,
        )

    def rows_of(j, lower):
        sky_block, start = place_of(j, lower)
        return pl.ds(pl.multiple_of(sky_block * BLOCK + start, ROWS), ROWS)

    def store(k, j, lower, a):
        rows = rows_of(j, lower)
        return pltpu.make_async_copy(ready.at[a, rows], out.at[a, rows], out_sem.at[a, k])

    def finish(j, _):
        for lower in (True, False):
            k = 2 * j + (0 if lower else 1)
            for copy in second_copies(k, j, lower):
                copy.wait_recv()
            source = second_a if lower else second_b
            count = ny if lower else nx
            rows = rows_of(j, lower)

            def summed(s):
                total = canvas[k, mine(lower) + s]
                for d in range(count - 1):
                    total = total + source[j, d, s]
                return total

            for s in range(half):
                canvas[k, mine(lower) + (1 - core) * half + s] = summed((1 - core) * half + s)
            last_copy(k, lower).start()
            for s in range(half):
                ready[core, rows, s * LANES : (s + 1) * LANES] = summed(core * half + s)
            store(k, j, lower, core).start()
            for copy in first_copies(k, j, lower):
                copy.wait_send()

        @pl.when(j >= LAG)
        def _():
            receive(j - LAG, 0)

        return 0

    def receive(j, _):
        for lower in (True, False):
            k = 2 * j + (0 if lower else 1)
            last_copy(k, lower).wait()
            rows = rows_of(j, lower)
            for s in range(half):
                ready[1 - core, rows, s * LANES : (s + 1) * LANES] = last[k, s]
            store(k, j, lower, 1 - core).start()
            for copy in second_copies(k, j, lower):
                copy.wait_send()
        return 0

    lax.fori_loop(0, pairs, finish, 0)
    lax.fori_loop(pairs - LAG, pairs, receive, 0)

    def stored(j, _):
        for lower in (True, False):
            for a in (core, 1 - core):
                store(2 * j + (0 if lower else 1), j, lower, a).wait()
        return 0

    lax.fori_loop(0, pairs, stored, 0)
    halo.wait_send()


def body(ny, nx, n_tile, images, beams, row_block, col_block, band, row_frac, col_frac):
    points, img_rows, width = images.shape
    blocks = img_rows // BLOCK
    col_tiles = width // LANES
    sky_tiles = SKY_COLS // LANES
    own = sky_tiles // (ny * nx)
    pairs = TILE_BLOCKS * PER_BLOCK
    chunks = 2 * pairs
    own_cols = SKY_COLS // (2 * ny * nx)
    most = max(nx, ny) - 1
    dma = pltpu.SemaphoreType.DMA
    smem = pl.BlockSpec(memory_space=pltpu.SMEM)
    summed = pl.pallas_call(
        functools.partial(kernel, ny, nx, n_tile),
        out_shape=jax.ShapeDtypeStruct((2, TILE_BLOCKS * BLOCK, own_cols), F32),
        in_specs=[pl.BlockSpec(memory_space=pl.ANY)] * 2 + [smem] * 5,
        out_specs=pl.BlockSpec(memory_space=pl.ANY),
        scratch_shapes=[
            pltpu.VMEM((2, points, img_rows, width), F32),
            pltpu.VMEM((4, BLOCK + 16, LANES), F32),
            pltpu.VMEM((2 * points * blocks * col_tiles + 1, TALL, LANES), F32),
            pltpu.VMEM((2, sky_tiles, 8, LANES), F32),
            pltpu.VMEM((2, sky_tiles, 8, LANES), F32),
            pltpu.VMEM((chunks, sky_tiles, ROWS, LANES), F32),
            pltpu.VMEM((chunks, sky_tiles, ROWS, LANES), F32),
            pltpu.VMEM((chunks, sky_tiles, ROWS, LANES), F32),
            pltpu.VMEM((pairs, nx - 1, sky_tiles // nx, ROWS, LANES), F32),
            pltpu.VMEM((pairs, ny - 1, sky_tiles // ny, ROWS, LANES), F32),
            pltpu.VMEM((pairs, ny - 1, own, ROWS, LANES), F32),
            pltpu.VMEM((pairs, nx - 1, own, ROWS, LANES), F32),
            pltpu.VMEM((chunks, own // 2, ROWS, LANES), F32),
            pltpu.VMEM((2, TILE_BLOCKS * BLOCK, own_cols), F32),
            dma((2, points * blocks)),
            dma((2,)),
            dma((2, chunks)),
            dma((2, chunks, most)),
            dma((2, chunks, most)),
            dma((2, chunks)),
            dma((2, chunks)),
        ],
        compiler_params=pltpu.CompilerParams(
            collective_id=0, has_side_effects=True, vmem_limit_bytes=67043328
        ),
        name="combine",
    )(images, beams, row_block, col_block, band, row_frac, col_frac)
    numer = summed[0]
    weight = summed[1]
    normalised = numer / jnp.maximum(weight, 0.05)
    return (numer, weight, normalised)


def solution(mesh):
    ny, nx = chip_grid(mesh.shape["pgroup"])
    return jax.shard_map(
        functools.partial(body, ny, nx, mesh.shape["tile"]),
        mesh=mesh,
        in_specs=(
            P(("pgroup", "tile"), None, None),
            P(("pgroup", "tile"), None, None),
            P(("pgroup", "tile")),
            P(("pgroup", "tile")),
            P(("pgroup", "tile"), None),
            P(("pgroup", "tile")),
            P(("pgroup", "tile")),
        ),
        out_specs=(P("tile", "pgroup"), P("tile", "pgroup"), P("tile", "pgroup")),
        check_vma=False,
    )
```

```python
import functools
import math

import jax
import jax.numpy as jnp
from jax import lax
from jax.experimental import pallas as pl
from jax.experimental.pallas import tpu as pltpu
from jax.sharding import PartitionSpec as P

TILE_BLOCKS = 4
SKY_COLS = 4096
HALO = 4
LANES = 128
BLOCK = 128
ROWS = 32
PER_BLOCK = BLOCK // (2 * ROWS)
TALL = BLOCK + 8
AHEAD = 1
LAG = 2
MESH = pl.DeviceIdType.MESH
F32 = jnp.float32


def chip_grid(groups):
    chips = groups // 2
    along_x = math.isqrt(chips)
    while chips % along_x:
        along_x -= 1
    return chips // along_x, along_x


def kernel(
    ny, nx, n_tile,
    images, beams, row_block, col_block, band, row_frac, col_frac,
    out,
    raw, mid, placed, halo_out, halo_in, give, take, canvas,
    first_a, first_b, second_a, second_b, last,
    ready,
    load_sem, halo_sem, swap_sem, first_sem, second_sem, last_sem, out_sem,
):
    points, img_rows, width = images.shape
    blocks = img_rows // BLOCK
    col_tiles = width // LANES
    sky_tiles = SKY_COLS // LANES
    own = sky_tiles // (ny * nx)
    half = own // 2
    pairs = TILE_BLOCKS * PER_BLOCK
    per_array = points * blocks * col_tiles
    empty = 2 * per_array

    me = lax.axis_index("pgroup")
    tile = lax.axis_index("tile")
    core = lax.rem(me, 2)
    chip = me // 2
    x = lax.rem(chip, nx)
    y = chip // nx
    partner = me + 1 - 2 * core
    x_peers = [(y * nx + lax.rem(x + d, nx)) * 2 + core for d in range(1, nx)]
    y_peers = [(lax.rem(y + d, ny) * nx + x) * 2 + core for d in range(1, ny)]
    after = lax.rem(tile + 1, n_tile)
    before = lax.rem(tile + n_tile - 1, n_tile)

    loads = {}
    for b in reversed(range(blocks)):
        for p in range(points):
            for which, source in enumerate((images, beams)):
                rows = pl.ds(b * BLOCK, BLOCK)
                copy = pltpu.make_async_copy(
                    source.at[p, rows], raw.at[which, p, rows], load_sem.at[which, p * blocks + b]
                )
                copy.start()
                loads[which, p, b] = copy

    barrier = pltpu.get_barrier_semaphore()
    near = [{"pgroup": q} for q in [partner] + x_peers + y_peers]
    near += [{"tile": after}, {"tile": before}]
    for device in near:
        pl.semaphore_signal(barrier, inc=1, device_id=device, device_id_type=MESH)

    placed[empty] = jnp.zeros((TALL, LANES), F32)
    for slot in range(4):
        mid[slot, :8] = jnp.zeros((8, LANES), F32)
        mid[slot, 8 + BLOCK :] = jnp.zeros((8, LANES), F32)
    last_lane = lax.broadcasted_iota(jnp.int32, (BLOCK, LANES), 1) == LANES - 1

    def interpolate(a, fresh, some):
        for b in some:
            for p in range(points):
                f = row_frac[p]
                g = col_frac[p]
                if fresh:
                    loads[0, p, b].wait()
                    loads[1, p, b].wait()
                shift = band[p, b]
                rows = pl.ds(b * BLOCK, BLOCK)

                def some_tiles(step, _, p=p, b=b, f=f, g=g, shift=shift, rows=rows):
                    for sub in range(4):
                        t = 4 * step + sub
                        lanes = pl.ds(pl.multiple_of(t * LANES, LANES), LANES)
                        here = raw[1, p, rows, lanes] * raw[a, p, rows, lanes]
                        if sub == 0:
                            left = pl.ds(pl.multiple_of(jnp.maximum(t - 1, 0) * LANES, LANES), LANES)
                            there = jnp.where(t > 0, 1.0, 0.0)
                            prior = raw[1, p, rows, left] * raw[a, p, rows, left] * there
                        else:
                            left = pl.ds(pl.multiple_of((t - 1) * LANES, LANES), LANES)
                            prior = raw[1, p, rows, left] * raw[a, p, rows, left]
                        moved = pltpu.roll(jnp.where(last_lane, prior, here), 1, 1)
                        mid[sub, 8 : 8 + BLOCK] = (1.0 - g) * here + g * moved
                        low = mid[sub, pl.ds(8 - shift, TALL)]
                        high = mid[sub, pl.ds(7 - shift, TALL)]
                        index = a * per_array + (p * blocks + b) * col_tiles + t
                        placed[index] = (1.0 - f) * low + f * high
                    return 0

                lax.fori_loop(0, col_tiles // 4, some_tiles, 0)

    def where_placed(a, p, sky_block, sky_tile):
        b = sky_block - (row_block[p] - tile * TILE_BLOCKS)
        t = sky_tile - col_block[p]
        inside = (b >= 0) & (b < blocks) & (t >= 0) & (t < col_tiles)
        index = a * per_array + (p * blocks + b) * col_tiles + t
        return jnp.where(inside, index, empty)

    def slot_of(sky_tile, x_major):
        if not x_major:
            return sky_tile
        owner = sky_tile // own
        return (lax.rem(owner, nx) * ny + owner // nx) * own + lax.rem(sky_tile, own)

    def place_of(m, lower):
        m = jnp.int32(m)
        sky_block = TILE_BLOCKS - 1 - m // PER_BLOCK
        turn = lax.rem(m, PER_BLOCK)
        start = BLOCK - ROWS * (2 * turn + (1 if lower else 2))
        return sky_block, pl.multiple_of(start, ROWS)

    def gather(a, m, sky_tile, lower):
        sky_block, start = place_of(m, lower)
        total = None
        for p in range(points):
            term = placed[where_placed(a, p, sky_block, sky_tile), pl.ds(start, ROWS)]
            total = term if total is None else total + term
        if lower:
            return total, None
        top = total[:8]
        for p in range(points):
            index = jnp.where(start == 0, where_placed(a, p, sky_block - 1, sky_tile), empty)
            top = top + placed[index, BLOCK:TALL]
        return total, top

    def border(sky_tile, _):
        for a in range(2):
            top = None
            for p in range(points):
                term = placed[where_placed(a, p, TILE_BLOCKS - 1, sky_tile), BLOCK:TALL]
                top = term if top is None else top + term
            halo_out[a, sky_tile] = top
        return 0

    halo = pltpu.make_async_remote_copy(
        halo_out, halo_in, halo_sem.at[0], halo_sem.at[1],
        device_id={"tile": after}, device_id_type=MESH,
    )

    def swap(k):
        return pltpu.make_async_remote_copy(
            give.at[k], take.at[k], swap_sem.at[0, k], swap_sem.at[1, k],
            device_id={"pgroup": partner}, device_id_type=MESH,
        )

    def build(k, j, lower):
        other = 1 - core

        def one(sky_tile, _):
            total, top = gather(other, j, sky_tile, lower)
            slot = slot_of(sky_tile, lower)
            give[k, slot] = total
            if top is not None:
                give[k, slot, :8] = top
            return 0

        lax.fori_loop(0, sky_tiles, one, 0, unroll=2)
        if not lower:
            @pl.when(jnp.int32(j) == pairs - 1)
            def _():
                halo.wait_recv()
                use = jnp.where(tile > 0, 1.0, 0.0)

                def add(s, _):
                    give[k, s, :8] += use * halo_in[other, s]
                    return 0

                lax.fori_loop(0, sky_tiles, add, 0, unroll=4)
        swap(k).start()

    def first_copies(k, j, lower):
        copies = []
        count, at, peers = (nx, x, x_peers) if lower else (ny, y, y_peers)
        size = sky_tiles // count
        target = first_a if lower else first_b
        for d in range(1, count):
            to = lax.rem(at + d, count)
            copies.append(pltpu.make_async_remote_copy(
                canvas.at[k, pl.ds(to * size, size)], target.at[j, d - 1],
                first_sem.at[0, k, d - 1], first_sem.at[1, k, d - 1],
                device_id={"pgroup": peers[d - 1]}, device_id_type=MESH,
            ))
        return copies

    def second_copies(k, j, lower):
        copies = []
        count, at, peers = (ny, y, y_peers) if lower else (nx, x, x_peers)
        base = (x * ny if lower else y * nx) * own
        target = second_a if lower else second_b
        for d in range(1, count):
            to = lax.rem(at + d, count)
            copies.append(pltpu.make_async_remote_copy(
                canvas.at[k, pl.ds(base + to * own, own)], target.at[j, d - 1],
                second_sem.at[0, k, d - 1], second_sem.at[1, k, d - 1],
                device_id={"pgroup": peers[d - 1]}, device_id_type=MESH,
            ))
        return copies

    def combine(k, j, lower):
        swap(k).wait_recv()

        def one(sky_tile, _):
            total, top = gather(core, j, sky_tile, lower)
            slot = slot_of(sky_tile, lower)
            canvas[k, slot] = total + take[k, slot]
            if top is not None:
                canvas[k, slot, :8] = top + take[k, slot, :8]
            return 0

        lax.fori_loop(0, sky_tiles, one, 0, unroll=2)
        if not lower:
            @pl.when(jnp.int32(j) == pairs - 1)
            def _():
                use = jnp.where(tile > 0, 1.0, 0.0)

                def add(s, _):
                    canvas[k, s, :8] += use * halo_in[core, s]
                    return 0

                lax.fori_loop(0, sky_tiles, add, 0, unroll=4)
        for copy in first_copies(k, j, lower):
            copy.start()

    groups = [[blocks - 1], list(reversed(range(blocks - 1)))]
    interpolate(1 - core, True, groups[0])
    pl.semaphore_wait(barrier, len(near))
    build(0, 0, True)
    build(1, 0, False)
    interpolate(core, False, groups[0])
    combine(0, 0, True)
    combine(1, 0, False)
    interpolate(1 - core, True, groups[1])
    for m in range(1, 1 + AHEAD):
        build(2 * m, m, True)
        build(2 * m + 1, m, False)
    interpolate(core, False, groups[1])

    def spread(j, _):
        for lower in (True, False):
            combine(2 * j + (0 if lower else 1), j, lower)

        @pl.when(j == 1)
        def _():
            lax.fori_loop(0, sky_tiles, border, 0)
            halo.start()

        @pl.when(j < pairs - AHEAD)
        def _():
            for lower in (True, False):
                build(2 * (j + AHEAD) + (0 if lower else 1), j + AHEAD, lower)
        return 0

    lax.fori_loop(1, pairs, spread, 0)

    def middle(j, _):
        for lower in (True, False):
            k = 2 * j + (0 if lower else 1)
            copies = first_copies(k, j, lower)
            for copy in copies:
                copy.wait_recv()
            count, at = (nx, x) if lower else (ny, y)
            size = sky_tiles // count
            source = first_a if lower else first_b

            def one(s, _):
                total = canvas[k, at * size + s]
                for d in range(count - 1):
                    total = total + source[j, d, s]
                canvas[k, at * size + s] = total
                return 0

            lax.fori_loop(0, size, one, 0, unroll=2)
            for copy in second_copies(k, j, lower):
                copy.start()
            swap(k).wait_send()
        return 0

    lax.fori_loop(0, pairs, middle, 0)

    def mine(lower):
        return (x * ny + y if lower else y * nx + x) * own

    def last_copy(k, lower):
        return pltpu.make_async_remote_copy(
            canvas.at[k, pl.ds(mine(lower) + (1 - core) * half, half)], last.at[k],
            last_sem.at[0, k], last_sem.at[1, k],
            device_id={"pgroup": partner}, device_id_type=MESH,
        )

    def rows_of(j, lower):
        sky_block, start = place_of(j, lower)
        return pl.ds(pl.multiple_of(sky_block * BLOCK + start, ROWS), ROWS)

    def store(k, j, lower, a):
        rows = rows_of(j, lower)
        return pltpu.make_async_copy(ready.at[a, rows], out.at[a, rows], out_sem.at[a, k])

    def finish(j, _):
        for lower in (True, False):
            k = 2 * j + (0 if lower else 1)
            for copy in second_copies(k, j, lower):
                copy.wait_recv()
            source = second_a if lower else second_b
            count = ny if lower else nx
            rows = rows_of(j, lower)

            def summed(s):
                total = canvas[k, mine(lower) + s]
                for d in range(count - 1):
                    total = total + source[j, d, s]
                return total

            for s in range(half):
                canvas[k, mine(lower) + (1 - core) * half + s] = summed((1 - core) * half + s)
            last_copy(k, lower).start()
            for s in range(half):
                ready[core, rows, s * LANES : (s + 1) * LANES] = summed(core * half + s)
            store(k, j, lower, core).start()
            for copy in first_copies(k, j, lower):
                copy.wait_send()

        @pl.when(j >= LAG)
        def _():
            receive(j - LAG, 0)

        return 0

    def receive(j, _):
        for lower in (True, False):
            k = 2 * j + (0 if lower else 1)
            last_copy(k, lower).wait()
            rows = rows_of(j, lower)
            for s in range(half):
                ready[1 - core, rows, s * LANES : (s + 1) * LANES] = last[k, s]
            store(k, j, lower, 1 - core).start()
            for copy in second_copies(k, j, lower):
                copy.wait_send()
        return 0

    lax.fori_loop(0, pairs, finish, 0)
    lax.fori_loop(pairs - LAG, pairs, receive, 0)

    def stored(j, _):
        for lower in (True, False):
            for a in (core, 1 - core):
                store(2 * j + (0 if lower else 1), j, lower, a).wait()
        return 0

    lax.fori_loop(0, pairs, stored, 0)
    halo.wait_send()


def body(ny, nx, n_tile, images, beams, row_block, col_block, band, row_frac, col_frac):
    points, img_rows, width = images.shape
    blocks = img_rows // BLOCK
    col_tiles = width // LANES
    sky_tiles = SKY_COLS // LANES
    own = sky_tiles // (ny * nx)
    pairs = TILE_BLOCKS * PER_BLOCK
    chunks = 2 * pairs
    own_cols = SKY_COLS // (2 * ny * nx)
    most = max(nx, ny) - 1
    dma = pltpu.SemaphoreType.DMA
    smem = pl.BlockSpec(memory_space=pltpu.SMEM)
    summed = pl.pallas_call(
        functools.partial(kernel, ny, nx, n_tile),
        out_shape=jax.ShapeDtypeStruct((2, TILE_BLOCKS * BLOCK, own_cols), F32),
        in_specs=[pl.BlockSpec(memory_space=pl.ANY)] * 2 + [smem] * 5,
        out_specs=pl.BlockSpec(memory_space=pl.ANY),
        scratch_shapes=[
            pltpu.VMEM((2, points, img_rows, width), F32),
            pltpu.VMEM((4, BLOCK + 16, LANES), F32),
            pltpu.VMEM((2 * points * blocks * col_tiles + 1, TALL, LANES), F32),
            pltpu.VMEM((2, sky_tiles, 8, LANES), F32),
            pltpu.VMEM((2, sky_tiles, 8, LANES), F32),
            pltpu.VMEM((chunks, sky_tiles, ROWS, LANES), F32),
            pltpu.VMEM((chunks, sky_tiles, ROWS, LANES), F32),
            pltpu.VMEM((chunks, sky_tiles, ROWS, LANES), F32),
            pltpu.VMEM((pairs, nx - 1, sky_tiles // nx, ROWS, LANES), F32),
            pltpu.VMEM((pairs, ny - 1, sky_tiles // ny, ROWS, LANES), F32),
            pltpu.VMEM((pairs, ny - 1, own, ROWS, LANES), F32),
            pltpu.VMEM((pairs, nx - 1, own, ROWS, LANES), F32),
            pltpu.VMEM((chunks, own // 2, ROWS, LANES), F32),
            pltpu.VMEM((2, TILE_BLOCKS * BLOCK, own_cols), F32),
            dma((2, points * blocks)),
            dma((2,)),
            dma((2, chunks)),
            dma((2, chunks, most)),
            dma((2, chunks, most)),
            dma((2, chunks)),
            dma((2, chunks)),
        ],
        compiler_params=pltpu.CompilerParams(
            collective_id=0, has_side_effects=True, vmem_limit_bytes=67043328
        ),
        name="combine",
    )(images, beams, row_block, col_block, band, row_frac, col_frac)
    numer = summed[0]
    weight = summed[1]
    normalised = numer / jnp.maximum(weight, 0.05)
    return (numer, weight, normalised)


def solution(mesh):
    ny, nx = chip_grid(mesh.shape["pgroup"])
    return jax.shard_map(
        functools.partial(body, ny, nx, mesh.shape["tile"]),
        mesh=mesh,
        in_specs=(
            P(("pgroup", "tile"), None, None),
            P(("pgroup", "tile"), None, None),
            P(("pgroup", "tile")),
            P(("pgroup", "tile")),
            P(("pgroup", "tile"), None),
            P(("pgroup", "tile")),
            P(("pgroup", "tile")),
        ),
        out_specs=(P("tile", "pgroup"), P("tile", "pgroup"), P("tile", "pgroup")),
        check_vma=False,
    )
```
